32 devices in a mesh: dp: 16 (over z, y, x), tensor: 2 (over core).
Axes of the slice: x: 2, y: 2, z: 4, core: 2. Of those that a mesh axis runs over, the one named last changes fastest.
Arguments:
- tokens: bfloat16 [16384, 640], P('dp'), may hold values from -6 to 6
- cotangent: bfloat16 [16384, 640], P('dp'), may hold values from -6 to 6
- lengths: int32 [16], P('dp'), may hold values from 256 to 1024, as said below
- pad_mask: int32 [16, 1024], P('dp'), may hold values 0 or 1
- w_qkv: bfloat16 [640, 3, 640], P(None, None, 'tensor'), may hold values from -0.25 to 0.25
- b_qkv: float32 [3, 640], P(None, 'tensor'), may hold values from -3 to 3
- w_out: bfloat16 [640, 640], P('tensor'), may hold values from -4 to 4
- b_out: float32 [640], replicated, may hold values from -3 to 3
- w_up: bfloat16 [640, 2560], P(None, 'tensor'), may hold values from -0.25 to 0.25
- b_up: float32 [2560], P('tensor'), may hold values from -3 to 3
- w_down: bfloat16 [2560, 640], P('tensor'), may hold values from -0.125 to 0.125
- b_down: float32 [640], replicated, may hold values from -3 to 3
- gain_one: float32 [640], replicated, may hold values from 0.25 to 1.75
- shift_one: float32 [640], replicated, may hold values from -3 to 3
- gain_two: float32 [640], replicated, may hold values from 0.25 to 1.75
- shift_two: float32 [640], replicated, may hold values from -3 to 3
Outputs:
- out_tokens: bfloat16 [16384, 640], P('dp')
- grad_tokens: float32 [16384, 640], P('dp')
- grad_w_qkv: float32 [640, 3, 640], P(None, None, 'tensor')
- grad_b_qkv: float32 [3, 640], P(None, 'tensor')
- grad_w_out: float32 [640, 640], P('tensor')
- grad_b_out: float32 [640], replicated
- grad_w_up: float32 [640, 2560], P(None, 'tensor')
- grad_b_up: float32 [2560], P('tensor')
- grad_w_down: float32 [2560, 640], P('tensor')
- grad_b_down: float32 [640], replicated
- grad_gain_one: float32 [640], replicated
- grad_shift_one: float32 [640], replicated
- grad_gain_two: float32 [640], replicated
- grad_shift_two: float32 [640], replicated
The draws below stay inside these ranges and needn't reach their ends.
Inputs may be any that keep to these rules, and one draw needn't show every extreme that they name: `lengths`: some window has exactly 1024 valid tokens and another exactly 256.
All inputs are finite; a program needn't handle non-finite values. No bound on the sum of `pad_mask` on one device may be relied on, other than what follows from the above.
Results may differ from the reference program's by a relative error of at most 0.012.
The reference program's roundings to bfloat16 on the way count: a program that leaves them out, or rounds other values in their place, can miss the bound.
Values sent between devices are 32-bit elements; how exact they have to be, the bound alone decides.
No kernel may reach another device: no remote copies, remote signals or barrier semaphores. Data moves between devices by JAX's collectives and lax.ppermute only.
A program may use at most 192 MiB of HBM per device.

```python
import jax
import jax.numpy as jnp
from jax import lax

D = 640
H = 20
HD = 32
FF = 2560
SEQ_LEN = 1024
WINDOWS = 16
TOKENS = 16384


def draw_lengths(key, part):
    key_base = jax.random.fold_in(key, 11)
    key_full = jax.random.fold_in(key, 12)
    key_short = jax.random.fold_in(key, 13)
    drawn = jax.random.randint(key_base, (WINDOWS,), SEQ_LEN // 4, SEQ_LEN + 1)
    full_slot = jax.random.randint(key_full, (), 0, WINDOWS)
    short_slot = (full_slot + 1 + jax.random.randint(key_short, (), 0, WINDOWS - 1)) % WINDOWS
    slots = jnp.arange(WINDOWS)
    drawn = jnp.where(slots == full_slot, SEQ_LEN, drawn)
    drawn = jnp.where(slots == short_slot, SEQ_LEN // 4, drawn)
    return drawn.astype(jnp.int32)


def place_ends(values, stream_key, low, largest):
    longest = values.shape.index(max(values.shape))
    spots = []
    for shift in (0, 1):
        where = [jax.random.randint(jax.random.fold_in(stream_key, axis), (), 0, length) for axis, length in enumerate(values.shape)]
        where[longest] = (where[longest] + shift) % values.shape[longest]
        spots.append(tuple(where))
    return values.at[spots[0]].set(low).at[spots[1]].set(largest)


def block_levels(key, extent, pieces, low, top_value):
    gain = 1.0
    for dim, shards_of in pieces:
        draws = jax.random.uniform(jax.random.fold_in(jax.random.fold_in(key, 6), dim), (shards_of,), jnp.float32, low / len(pieces), top_value / len(pieces))
        gain = gain * jnp.repeat(jnp.exp(draws), extent[dim] // shards_of).reshape((-1,) + (1,) * (len(extent) - 1 - dim))
    return gain


def bell_draw(own_key, extent, spread, limit, pieces=(), held_as=jnp.bfloat16):
    values = spread * jax.random.normal(own_key, extent, jnp.float32)
    if pieces:
        values = values * block_levels(own_key, extent, pieces, -0.22, 0.18)
    return jnp.clip(values, -limit, limit).astype(held_as)


def setup_inputs(seed: int = 0) -> dict:
    streams_of = jax.random.split(jax.random.key(seed), 17)
    return {
        "tokens": bell_draw(streams_of[0], (TOKENS, D), 1.0, 6.0, ((0, 16),)),
        "cotangent": bell_draw(streams_of[1], (TOKENS, D), 1.0, 6.0, ((0, 16),)),
        "lengths": draw_lengths(jax.random.fold_in(streams_of[16], 71), 0),
        "pad_mask": place_ends((jax.random.randint(streams_of[3], (WINDOWS, SEQ_LEN), 0, 16) < 15).astype(jnp.int32), jax.random.fold_in(streams_of[3], 1), 0, 1),
        "w_qkv": bell_draw(streams_of[4], (D, 3, D), D ** -0.5, 0.25, ((2, 2),)),
        "b_qkv": bell_draw(streams_of[5], (3, D), 0.3, 3.0, ((1, 2),), jnp.float32),
        "w_out": bell_draw(streams_of[6], (D, D), 2 ** -0.5, 4.0, ((0, 2),)),
        "b_out": bell_draw(streams_of[7], (D,), 0.5, 3.0, (), jnp.float32),
        "w_up": bell_draw(streams_of[8], (D, FF), D ** -0.5, 0.25, ((1, 2),)),
        "b_up": bell_draw(streams_of[9], (FF,), 0.5, 3.0, ((0, 2),), jnp.float32),
        "w_down": bell_draw(streams_of[10], (FF, D), FF ** -0.5, 0.125, ((0, 2),)),
        "b_down": bell_draw(streams_of[11], (D,), 0.5, 3.0, (), jnp.float32),
        "gain_one": jnp.clip(1.0 + 0.15 * jax.random.normal(streams_of[12], (D,), jnp.float32), 0.25, 1.75),
        "shift_one": bell_draw(streams_of[13], (D,), 0.5, 3.0, (), jnp.float32),
        "gain_two": jnp.clip(1.0 + 0.15 * jax.random.normal(streams_of[14], (D,), jnp.float32), 0.25, 1.75),
        "shift_two": bell_draw(streams_of[15], (D,), 0.5, 3.0, (), jnp.float32),
    }


@jax.custom_vjp
def low(v):
    return lax.optimization_barrier(v.astype(jnp.bfloat16)).astype(jnp.float32)

@jax.custom_vjp
def low_back(v):
    return v

def low_keep(v):
    return (low(v), None)

def low_pass(kept, grad):
    return (grad,)

def back_keep(v):
    return (v, None)

def back_low(kept, grad):
    return (low(grad),)
low.defvjp(low_keep, low_pass)
low_back.defvjp(back_keep, back_low)
EPSILON = 1e-05
ROOT_HALF = 0.7071067811865476
HIGHEST = lax.Precision.HIGHEST

def matmul(left, right):
    return jnp.dot(left, right, precision=HIGHEST, preferred_element_type=jnp.float32)

def norm_rows(values, gain_vec, shift_vec):
    centre = lax.optimization_barrier(jnp.mean(values, axis=1, keepdims=True))
    shifted = values - centre
    inverse = lax.rsqrt(lax.optimization_barrier(jnp.mean(shifted * shifted, axis=1, keepdims=True)) + EPSILON)
    return shifted * inverse * gain_vec + shift_vec

def rotate(values, cosine_table, sine_table):
    half_size = values.shape[-1] // 2
    lower_half = values[..., :half_size]
    upper_half = values[..., half_size:]
    turned = jnp.concatenate([-upper_half, lower_half], axis=-1)
    return values * cosine_table + turned * sine_table

def block_forward(inputs, params, cosine_table, sine_table, visible):
    w_qkv, b_qkv, w_out, b_out, w_up, b_up, w_down, b_down, gain_one, shift_one, gain_two, shift_two = params
    hidden_one = low(norm_rows(inputs, gain_one, shift_one))
    projected = matmul(hidden_one, w_qkv.reshape(D, 3 * D)) + b_qkv.reshape(3 * D)
    projected = low_back(projected).reshape(SEQ_LEN, 3, H, HD)
    query_rows = low(rotate(projected[:, 0], cosine_table, sine_table) * HD ** (-0.5))
    key_rows = low(rotate(projected[:, 1], cosine_table, sine_table))
    value_rows = low(projected[:, 2])
    scores = low_back(jnp.einsum('qhd,khd->hqk', query_rows, key_rows, precision=HIGHEST))
    scores = jnp.where(visible[None, None, :], scores, -1000000000.0)
    row_peak = lax.optimization_barrier(jnp.max(scores, axis=2, keepdims=True))
    powers = jnp.exp(scores - row_peak)
    chances = low(powers / lax.optimization_barrier(jnp.sum(powers, axis=2, keepdims=True)))
    attended = jnp.einsum('hqk,khd->qhd', chances, value_rows, precision=HIGHEST).reshape(SEQ_LEN, D)
    attended = low_back(low(attended))
    resid_one = inputs + low_back(matmul(attended, w_out) + b_out)
    hidden_two = low(norm_rows(resid_one, gain_two, shift_two))
    upward = low_back(matmul(hidden_two, w_up) + b_up)
    activated = low(0.5 * upward * (1.0 + lax.erf(upward * ROOT_HALF)))
    return resid_one + low_back(matmul(activated, w_down) + b_down)

def reference(tokens, cotangent, lengths, pad_mask, w_qkv, b_qkv, w_out, b_out, w_up, b_up, w_down, b_down, gain_one, shift_one, gain_two, shift_two):
    params = jax.tree.map(lambda member: member.astype(jnp.float32), (w_qkv, b_qkv, w_out, b_out, w_up, b_up, w_down, b_down, gain_one, shift_one, gain_two, shift_two))
    windows = tokens.astype(jnp.float32).reshape(-1, SEQ_LEN, D)
    grad_rows = cotangent.astype(jnp.float32).reshape(-1, SEQ_LEN, D)
    half_size = HD // 2
    frequency = 10000.0 ** (-(2.0 * jnp.arange(half_size, dtype=jnp.float32)) / HD)
    places = jnp.arange(SEQ_LEN, dtype=jnp.int32)
    position = places.astype(jnp.float32)
    angles = position[:, None] * frequency[None, :]
    cosine_table = jnp.concatenate([jnp.cos(angles), jnp.cos(angles)], axis=-1)[:, None, :]
    sine_table = jnp.concatenate([jnp.sin(angles), jnp.sin(angles)], axis=-1)[:, None, :]

    def one_window(running, packed):
        window, grad_window, length, mask_row = packed
        visible = (places < length) & (mask_row == 1) | (places == 0)
        result, pullback = jax.vjp(lambda inputs, weights: block_forward(inputs, weights, cosine_table, sine_table, visible), window, params)
        grad_input, grad_params = pullback(grad_window)
        running = jax.tree.map(jnp.add, running, grad_params)
        return (running, (result.astype(jnp.bfloat16), grad_input))
    empty_sums = jax.tree.map(jnp.zeros_like, params)
    totals, (results, grad_inputs) = lax.scan(one_window, empty_sums, (windows, grad_rows, lengths, pad_mask))
    return (results.reshape(-1, D), grad_inputs.reshape(-1, D), totals[0], totals[1], totals[2], totals[3], totals[4], totals[5], totals[6], totals[7], totals[8], totals[9], totals[10], totals[11])
```

```python
import functools
import math

import jax
import jax.numpy as jnp
import numpy as np
from jax import lax
from jax.experimental import pallas as pl
from jax.experimental.pallas import tpu as pltpu
from jax.sharding import PartitionSpec as P

HD = 32
HALF = HD // 2
EPSILON = 1e-05
ROOT_HALF = 0.7071067811865476
ROOT_TWO_PI = 2.5066282746310002
LOG2E = math.log2(math.e)
HIDDEN_BIAS = -1e30
SAFE_POWER = 96.0
f32 = jnp.float32
bf16 = jnp.bfloat16


def dot_nn(a, b):
    return lax.dot_general(a, b, (((1,), (0,)), ((), ())), preferred_element_type=f32)


def dot_nt(a, b):
    return lax.dot_general(a, b, (((1,), (1,)), ((), ())), preferred_element_type=f32)


def dot_tn(a, b):
    return lax.dot_general(a, b, (((0,), (0,)), ((), ())), preferred_element_type=f32)


def normalize(values):
    centre = jnp.mean(values, axis=1, keepdims=True)
    shifted = values - centre
    inverse = lax.rsqrt(jnp.mean(shifted * shifted, axis=1, keepdims=True) + EPSILON)
    return shifted * inverse, inverse


def norm_back(grad_normed, normed, inverse, gain_vec):
    scaled = grad_normed * gain_vec
    first_mean = jnp.mean(scaled, axis=1, keepdims=True)
    second_mean = jnp.mean(scaled * normed, axis=1, keepdims=True)
    return inverse * (scaled - first_mean - normed * second_mean)


def split_three(values):
    first = values.astype(bf16)
    rest = values - first.astype(f32)
    second = rest.astype(bf16)
    third = (rest - second.astype(f32)).astype(bf16)
    return first, second, third


def stack_rows(*rows):
    count = rows[0].shape[1]
    place = lax.broadcasted_iota(jnp.int32, (16, count), 0)
    out = jnp.zeros((16, count), f32)
    for index, row in enumerate(rows):
        out = jnp.where(place == index, row, out)
    return out.astype(bf16)


def rope_rows(values, cosine, sine):
    heads = values.reshape(-1, 2, HALF, values.shape[1])
    lower, upper = heads[:, 0], heads[:, 1]
    turned = jnp.stack([lower * cosine - upper * sine, upper * cosine + lower * sine], axis=1)
    return turned.reshape(values.shape)


def rope_back_rows(values, cosine, sine):
    heads = values.reshape(-1, 2, HALF, values.shape[1])
    lower, upper = heads[:, 0], heads[:, 1]
    turned = jnp.stack([lower * cosine + upper * sine, upper * cosine - lower * sine], axis=1)
    return turned.reshape(values.shape)


def spread_chunks(total_ref, keep_ref, send_ref, me, count):
    size = total_ref.shape[0] // count
    half = count // 2
    for place in range(count):
        chunk = jnp.bitwise_xor(me, place)
        rows = total_ref[pl.ds(pl.multiple_of(chunk * size, size), size), :]
        target = keep_ref if place < half else send_ref
        start = (place % half) * size
        target[start : start + size, :] = rows


def front_kernel(
    block,
    steps,
    length_ref,
    tokens_ref,
    w_ref,
    b_ref,
    gain_ref,
    shift_ref,
    cos_ref,
    sin_ref,
    mask_ref,
    w_out_ref,
    hidden_ref,
    q_ref,
    k_ref,
    v_ref,
    att_ref,
    lse_ref,
    bias_ref,
    mix_ref,
):
    step = pl.program_id(0)
    seq_len = q_ref.shape[1]
    width = q_ref.shape[0]
    per_step = 2
    query_scale = HD ** (-0.5)

    @pl.when(step == 0)
    def _():
        place = lax.broadcasted_iota(jnp.int32, (1, seq_len), 1)
        visible = (place < length_ref[0]) & (mask_ref[...] == 1) | (place == 0)
        bias_ref[...] = jnp.where(visible, 0.0, HIDDEN_BIAS)

    @pl.when(step < steps)
    def _():
        normed, _ = normalize(tokens_ref[...].astype(f32))
        hidden = (normed * gain_ref[...] + shift_ref[...]).astype(bf16)
        hidden_ref[...] = hidden
        projected = dot_nt(w_ref[...].reshape(3 * width, w_ref.shape[2]), hidden)
        columns = pl.ds(pl.multiple_of(step * block, block), block)
        parts = []
        for index in range(3):
            column = jnp.broadcast_to(b_ref[index : index + 1, :], (128, width)).T
            column = jnp.concatenate([column] * (block // 128), axis=1)
            parts.append(projected[index * width : (index + 1) * width] + column)
        cosine, sine = cos_ref[...], sin_ref[...]
        q_ref[:, columns] = (rope_rows(parts[0], cosine, sine) * query_scale).astype(bf16)
        k_ref[:, columns] = rope_rows(parts[1], cosine, sine).astype(bf16)
        v_ref[:, columns] = parts[2].astype(bf16)

    @pl.when(step >= steps)
    def _():
        ones = jnp.ones((1, seq_len), f32)
        key_extra = stack_rows(bias_ref[...])
        value_extra = stack_rows(ones)
        query_extra = stack_rows(ones)
        first_head = (step - steps) * per_step
        queries, keys, values, bounds = [], [], [], []
        for index in range(per_step):
            rows = pl.ds(pl.multiple_of((first_head + index) * HD, HD), HD)
            key = k_ref[rows, :]
            query = q_ref[rows, :].astype(f32) * LOG2E
            key_wide = key.astype(f32)
            bounds.append(
                jnp.max(jnp.sum(query * query, axis=0, keepdims=True))
                * jnp.max(jnp.sum(key_wide * key_wide, axis=0, keepdims=True))
            )
            queries.append(jnp.concatenate([*split_three(query), query_extra], axis=0))
            keys.append(jnp.concatenate([key, key, key, key_extra], axis=0))
            values.append(jnp.concatenate([v_ref[rows, :], value_extra], axis=0))
        bound = bounds[0]
        for other in bounds[1:]:
            bound = jnp.maximum(bound, other)

        def attend(shifted):
            size = min(512, seq_len)
            for index in range(per_step):
                head = first_head + index
                rows = pl.ds(pl.multiple_of(head * HD, HD), HD)
                for start in range(0, seq_len, size):
                    part = slice(start, start + size)
                    scores = dot_tn(keys[index], queries[index][:, part])
                    if shifted:
                        peak = jnp.max(scores, axis=0, keepdims=True)
                        powers = jnp.exp2(scores - peak)
                    else:
                        peak = 0.0
                        powers = jnp.exp2(scores)
                    summed = dot_nn(values[index], powers.astype(bf16))
                    total = summed[HD : HD + 1, :]
                    att_ref[rows, part] = (summed[:HD] * (1.0 / total)).astype(bf16)
                    lse_ref[head, :, part] = peak + jnp.log(total) * LOG2E

        small = bound < SAFE_POWER * SAFE_POWER

        @pl.when(small)
        def _():
            attend(False)

        @pl.when(jnp.logical_not(small))
        def _():
            attend(True)

    @pl.when(step == pl.num_programs(0) - 1)
    def _():
        mix_ref[...] = dot_tn(att_ref[...], w_out_ref[...])


def const_spec(shape, index=None):
    where = tuple(index) if index is not None else (0,) * len(shape)
    return pl.BlockSpec(shape, lambda *_: where, pipeline_mode=pl.Buffered(1))


def out_spec(shape):
    where = (0,) * len(shape)
    return pl.BlockSpec(shape, lambda *_: where)


def front(tokens, lengths, pad_mask, w_t, b_qkv, w_out, gain_one, shift_one, cosine, sine):
    rows, model = tokens.shape
    width = w_t.shape[1]
    heads = width // HD
    block = min(256, rows)
    steps = rows // block
    clipped = lambda i: (jnp.minimum(i, steps - 1), 0)
    clipped_lanes = lambda i: (0, jnp.minimum(i, steps - 1))
    return pl.pallas_call(
        functools.partial(front_kernel, block, steps),
        grid=(steps + heads // 2,),
        in_specs=[
            pl.BlockSpec(memory_space=pltpu.SMEM),
            pl.BlockSpec((block, model), clipped),
            const_spec(w_t.shape),
            const_spec(b_qkv.shape),
            const_spec((1, model)),
            const_spec((1, model)),
            pl.BlockSpec((HALF, block), clipped_lanes),
            pl.BlockSpec((HALF, block), clipped_lanes),
            const_spec(pad_mask.shape),
            const_spec(w_out.shape),
        ],
        out_specs=[
            pl.BlockSpec((block, model), clipped),
            out_spec((width, rows)),
            out_spec((width, rows)),
            out_spec((width, rows)),
            out_spec((width, rows)),
            out_spec((heads, 1, rows)),
            out_spec((1, rows)),
            out_spec((rows, model)),
        ],
        out_shape=[
            jax.ShapeDtypeStruct((rows, model), bf16),
            jax.ShapeDtypeStruct((width, rows), bf16),
            jax.ShapeDtypeStruct((width, rows), bf16),
            jax.ShapeDtypeStruct((width, rows), bf16),
            jax.ShapeDtypeStruct((width, rows), bf16),
            jax.ShapeDtypeStruct((heads, 1, rows), f32),
            jax.ShapeDtypeStruct((1, rows), f32),
            jax.ShapeDtypeStruct((rows, model), f32),
        ],
        compiler_params=pltpu.CompilerParams(vmem_limit_bytes=32 << 20),
        cost_estimate=pl.CostEstimate(
            flops=20 * 10**9, bytes_accessed=10 << 20, transcendentals=10 << 20
        ),
        name="front",
    )(lengths, tokens, w_t, b_qkv, gain_one, shift_one, cosine, sine, pad_mask, w_out)


def mlp_kernel(first, count, *refs):
    if first:
        (me_ref, tokens_ref, own_ref, other_ref, b_out_ref, gain_ref, shift_ref) = refs[:7]
        refs = refs[7:]
    else:
        (me_ref, hidden_ref, down_in_ref, hid_in_ref) = refs[:4]
        refs = refs[4:]
    cot_ref, w_up_ref, b_up_ref, w_down_ref = refs[:4]
    refs = refs[4:]
    if first:
        resid_ref, hidden_ref = refs[:2]
        refs = refs[2:]
    (down_ref, hid_ref, wd_keep, wd_send, wu_keep, wu_send, b_up_sum, wd_total, wu_total) = refs[:9]
    step = pl.program_id(0)

    @pl.when(step == 0)
    def _():
        wd_total[...] = jnp.zeros_like(wd_total)
        wu_total[...] = jnp.zeros_like(wu_total)
        b_up_sum[...] = jnp.zeros_like(b_up_sum)

    if first:
        resid = tokens_ref[...].astype(f32) + ((own_ref[...] + other_ref[...]) + b_out_ref[...])
        resid_ref[...] = resid
        normed, _ = normalize(resid)
        hidden = (normed * gain_ref[...] + shift_ref[...]).astype(bf16)
        hidden_ref[...] = hidden
    else:
        hidden = hidden_ref[...]
    cot = cot_ref[...]
    w_up, w_down = w_up_ref[...], w_down_ref[...]
    upward = dot_nn(hidden, w_up) + b_up_ref[...]
    error_part = lax.erf(upward * ROOT_HALF)
    activated = (0.5 * upward * (1.0 + error_part)).astype(bf16)
    wd_total[...] += dot_tn(activated, cot)
    grad_act = dot_nt(cot, w_down)
    slope = 0.5 * (1.0 + error_part) + upward * jnp.exp(-0.5 * upward * upward) / ROOT_TWO_PI
    grad_up = (grad_act * slope).astype(bf16)
    wu_total[...] += dot_tn(hidden, grad_up)
    b_up_sum[...] += jnp.sum(grad_up.astype(f32), axis=0, keepdims=True)
    down = dot_nn(activated, w_down)
    hid = dot_nt(grad_up, w_up)
    if not first:
        down = down + down_in_ref[...]
        hid = hid + hid_in_ref[...]
    down_ref[...] = down
    hid_ref[...] = hid

    @pl.when(step == pl.num_programs(0) - 1)
    def _():
        spread_chunks(wd_total, wd_keep, wd_send, me_ref[0], count)
        spread_chunks(wu_total, wu_keep, wu_send, me_ref[1], count)


def mlp(first, half, count, me, extras, cotangent, w_up, b_up, w_down):
    rows, model = cotangent.shape
    hidden_half = w_up.shape[1] // 2
    block = min(256, rows)
    row_spec = pl.BlockSpec((block, model), lambda i: (i, 0))
    vec_spec = const_spec((1, model))
    in_specs = [pl.BlockSpec(memory_space=pltpu.SMEM)]
    in_specs += [row_spec] * 3 + ([vec_spec] * 3 if first else [])
    in_specs += [
        row_spec,
        const_spec((model, hidden_half), (0, half)),
        const_spec((1, hidden_half), (0, half)),
        const_spec((hidden_half, model), (half, 0)),
    ]
    rows_f32 = jax.ShapeDtypeStruct((rows, model), f32)
    rows_b16 = jax.ShapeDtypeStruct((rows, model), bf16)
    down_half = jax.ShapeDtypeStruct((hidden_half // 2, model), f32)
    up_half = jax.ShapeDtypeStruct((model // 2, hidden_half), f32)
    out_shape = ([rows_f32, rows_b16] if first else []) + [rows_f32, rows_f32]
    out_specs = [row_spec] * len(out_shape)
    out_shape += [down_half, down_half, up_half, up_half]
    out_shape += [jax.ShapeDtypeStruct((1, hidden_half), f32)]
    out_specs += [out_spec(s.shape) for s in out_shape[len(out_specs) :]]
    return pl.pallas_call(
        functools.partial(mlp_kernel, first, count),
        grid=(rows // block,),
        in_specs=in_specs,
        out_specs=out_specs,
        out_shape=out_shape,
        scratch_shapes=[
            pltpu.VMEM((hidden_half, model), f32),
            pltpu.VMEM((model, hidden_half), f32),
        ],
        compiler_params=pltpu.CompilerParams(vmem_limit_bytes=40 << 20),
        cost_estimate=pl.CostEstimate(
            flops=6 * 2 * rows * model * hidden_half,
            bytes_accessed=20 << 20,
            transcendentals=2 * rows * hidden_half,
        ),
        name="mlp_a" if first else "mlp_b",
    )(me, *extras, cotangent, w_up, b_up, w_down)


def middle_kernel(
    resid_ref,
    own_ref,
    other_ref,
    cot_ref,
    gain_ref,
    w_out_ref,
    grad_resid_ref,
    low_ref,
    grad_att_ref,
    sums_ref,
):
    step = pl.program_id(0)

    @pl.when(step == 0)
    def _():
        sums_ref[...] = jnp.zeros_like(sums_ref)

    normed, inverse = normalize(resid_ref[...])
    grad_hidden = own_ref[...] + other_ref[...]
    cot = cot_ref[...].astype(f32)
    grad_resid = cot + norm_back(grad_hidden, normed, inverse, gain_ref[...])
    low = grad_resid.astype(bf16)
    grad_resid_ref[...] = grad_resid
    low_ref[...] = low
    grad_att_ref[...] = dot_nt(w_out_ref[...], low).astype(bf16)
    sums_ref[0:1, :] += jnp.sum(grad_hidden * normed, axis=0, keepdims=True)
    sums_ref[1:2, :] += jnp.sum(grad_hidden, axis=0, keepdims=True)
    sums_ref[2:3, :] += jnp.sum(low.astype(f32), axis=0, keepdims=True)
    sums_ref[3:4, :] += jnp.sum(cot, axis=0, keepdims=True)


def middle(resid, own, other, cotangent, gain_two, w_out):
    rows, model = resid.shape
    width = w_out.shape[0]
    block = min(256, rows)
    row_spec = pl.BlockSpec((block, model), lambda i: (i, 0))
    return pl.pallas_call(
        middle_kernel,
        grid=(rows // block,),
        in_specs=[row_spec] * 4 + [const_spec((1, model)), const_spec(w_out.shape)],
        out_specs=[
            row_spec,
            row_spec,
            pl.BlockSpec((width, block), lambda i: (0, i)),
            out_spec((8, model)),
        ],
        out_shape=[
            jax.ShapeDtypeStruct((rows, model), f32),
            jax.ShapeDtypeStruct((rows, model), bf16),
            jax.ShapeDtypeStruct((width, rows), bf16),
            jax.ShapeDtypeStruct((8, model), f32),
        ],
        compiler_params=pltpu.CompilerParams(vmem_limit_bytes=24 << 20),
        cost_estimate=pl.CostEstimate(
            flops=2 * rows * model * width, bytes_accessed=12 << 20, transcendentals=rows
        ),
        name="middle",
    )(resid, own, other, cotangent, gain_two, w_out)


def attend_back_kernel(first, count, *refs):
    (
        me_ref,
        q_ref,
        k_ref,
        v_ref,
        att_ref,
        grad_att_ref,
        lse_ref,
        bias_ref,
        cos_ref,
        sin_ref,
        w_ref,
        hidden_ref,
        low_ref,
    ) = refs[:13]
    refs = refs[13:]
    if not first:
        part_in_ref = refs[0]
        refs = refs[1:]
    keep_ref, send_ref, part_ref, b_ref, grad_sc, total_sc = refs
    step = pl.program_id(0)
    seq_len = q_ref.shape[1]
    width = q_ref.shape[0]
    query_scale = HD ** (-0.5)
    rows = pl.ds(pl.multiple_of(step * HD, HD), HD)
    ones = jnp.ones((1, seq_len), f32)
    key, value, query_all = k_ref[rows, :], v_ref[rows, :], q_ref[rows, :]
    keys = jnp.concatenate([key, key, key, stack_rows(bias_ref[...], ones, ones, ones)], axis=0)
    values = jnp.concatenate([value, stack_rows(ones, ones, ones)], axis=0)
    cosine, sine = cos_ref[...], sin_ref[...]
    grad_all = grad_att_ref[rows, :]
    log_all = -lse_ref[step]
    inner_all = -jnp.sum(
        grad_all.astype(f32) * att_ref[rows, :].astype(f32), axis=0, keepdims=True
    )
    grad_key = jnp.zeros((HD, seq_len), f32)
    grad_value = jnp.zeros((HD, seq_len), f32)
    grad_query = []
    size = min(512, seq_len)
    for start in range(0, seq_len, size):
        part = slice(start, start + size)
        query = query_all[:, part]
        logs = [piece.astype(f32) for piece in split_three(log_all[:, part])]
        queries = jnp.concatenate(
            [
                *split_three(query.astype(f32) * LOG2E),
                stack_rows(ones[:, :size], *logs),
            ],
            axis=0,
        )
        chances = jnp.exp2(dot_tn(keys, queries))
        grad_out = grad_all[:, part]
        inner = [piece.astype(f32) for piece in split_three(inner_all[:, part])]
        grads = jnp.concatenate([grad_out, stack_rows(*inner)], axis=0)
        grad_scores = (chances * dot_tn(values, grads)).astype(bf16)
        grad_value = grad_value + dot_nt(grad_out, chances.astype(bf16))
        grad_key = grad_key + dot_nt(query, grad_scores)
        grad_query.append(dot_nn(key, grad_scores))
    grad_query = jnp.concatenate(grad_query, axis=1) * query_scale
    grad_sc[0, rows, :] = rope_back_rows(grad_query, cosine, sine).astype(bf16)
    grad_sc[1, rows, :] = rope_back_rows(grad_key, cosine, sine).astype(bf16)
    grad_sc[2, rows, :] = grad_value.astype(bf16)

    @pl.when(step == pl.num_programs(0) - 1)
    def _():
        grads = grad_sc[...].reshape(3 * width, seq_len)
        total_sc[: 3 * width, :] = dot_nn(grads, hidden_ref[...])
        total_sc[3 * width :, :] = dot_nn(att_ref[...], low_ref[...])
        spread_chunks(total_sc, keep_ref, send_ref, me_ref[0], count)
        weights = w_ref[...].reshape(3 * width, w_ref.shape[2])
        part = dot_tn(grads, weights)
        if not first:
            part = part + part_in_ref[...]
        part_ref[...] = part
        b_ref[...] = dot_nt(jnp.ones((8, seq_len), bf16), grads)


def attend_back(first, half, count, me, rows_in, lse, bias, cosine, sine, w_t, hidden, low, part):
    width, rows = rows_in[0].shape
    width //= 2
    model = hidden.shape[1]
    heads = width // HD
    head_spec = const_spec((width, rows), (half, 0))
    in_specs = [pl.BlockSpec(memory_space=pltpu.SMEM)] + [head_spec] * 5
    in_specs += [
        const_spec((heads, 1, rows), (half, 0, 0)),
        const_spec((1, rows)),
        const_spec((HALF, rows)),
        const_spec((HALF, rows)),
        const_spec((3, width, model), (0, half, 0)),
        const_spec((rows, model)),
        const_spec((rows, model)),
    ]
    extra = []
    if not first:
        in_specs.append(const_spec((rows, model)))
        extra = [part]
    pack = jax.ShapeDtypeStruct((2 * width, model), f32)
    out_shape = [
        pack,
        pack,
        jax.ShapeDtypeStruct((rows, model), f32),
        jax.ShapeDtypeStruct((8, 3 * width), f32),
    ]
    return pl.pallas_call(
        functools.partial(attend_back_kernel, first, count),
        grid=(heads,),
        in_specs=in_specs,
        out_specs=[out_spec(s.shape) for s in out_shape],
        out_shape=out_shape,
        scratch_shapes=[
            pltpu.VMEM((3, width, rows), bf16),
            pltpu.VMEM((4 * width, model), f32),
        ],
        compiler_params=pltpu.CompilerParams(vmem_limit_bytes=40 << 20),
        cost_estimate=pl.CostEstimate(
            flops=14 * 10**9, bytes_accessed=10 << 20, transcendentals=5 << 20
        ),
        name="attend_back_a" if first else "attend_back_b",
    )(me, *rows_in, lse, bias, cosine, sine, w_t, hidden, low, *extra)


def last_kernel(tokens_ref, own_ref, other_ref, grad_resid_ref, gain_ref, grad_ref, sums_ref):
    step = pl.program_id(0)

    @pl.when(step == 0)
    def _():
        sums_ref[...] = jnp.zeros_like(sums_ref)

    normed, inverse = normalize(tokens_ref[...].astype(f32))
    grad_hidden = own_ref[...] + other_ref[...]
    grad_ref[...] = grad_resid_ref[...] + norm_back(grad_hidden, normed, inverse, gain_ref[...])
    sums_ref[0:1, :] += jnp.sum(grad_hidden * normed, axis=0, keepdims=True)
    sums_ref[1:2, :] += jnp.sum(grad_hidden, axis=0, keepdims=True)


def last(tokens, own, other, grad_resid, gain_one):
    rows, model = tokens.shape
    block = min(256, rows)
    row_spec = pl.BlockSpec((block, model), lambda i: (i, 0))
    return pl.pallas_call(
        last_kernel,
        grid=(rows // block,),
        in_specs=[row_spec] * 4 + [const_spec((1, model))],
        out_specs=[row_spec, out_spec((8, model))],
        out_shape=[
            jax.ShapeDtypeStruct((rows, model), f32),
            jax.ShapeDtypeStruct((8, model), f32),
        ],
        compiler_params=pltpu.CompilerParams(vmem_limit_bytes=24 << 20),
        cost_estimate=pl.CostEstimate(
            flops=20 * rows * model, bytes_accessed=12 << 20, transcendentals=rows
        ),
        name="last",
    )(tokens, own, other, grad_resid, gain_one)


def flip(values, bit, size):
    return lax.ppermute(values, "dp", [(i, i ^ (1 << bit)) for i in range(size)])


class Chain:
    def __init__(self, order, size, keep, send):
        self.order, self.size = order, size
        self.keep, self.send = keep, send

    def reduce(self):
        keep, send = self.keep, self.send
        for index, bit in enumerate(self.order):
            total = keep + flip(send, bit, self.size)
            if index + 1 < len(self.order):
                half = total.shape[0] // 2
                keep, send = total[:half], total[half:]
        for bit in range(len(self.order), self.size.bit_length() - 1):
            total = total + flip(total, bit, self.size)
        self.own = total

    def gather(self):
        own = self.own
        for bit in self.order[:0:-1]:
            own = jnp.concatenate([own, flip(own, bit, self.size)], axis=0)
        return own, flip(own, self.order[0], self.size)


def place_index(order):
    index = lax.axis_index("dp")
    out = jnp.zeros((), jnp.int32)
    for bit in order:
        out = out * 2 + jnp.bitwise_and(jnp.right_shift(index, bit), 1)
    return out


def assemble_kernel(kind, count, me_ref, *refs):
    pieces, rest = refs[:4], refs[4:]
    outs, sem = rest[:-1], rest[-1]
    half = count // 2
    size = pieces[0].shape[0] // half
    for wait in (False, True):
        for group in range(2):
            for place in range(count):
                chunk = jnp.bitwise_xor(me_ref[group], place)
                source = pieces[2 * group + place // half].at[
                    pl.ds((place % half) * size, size), :
                ]
                slot = sem.at[group * count + place]
                row = pl.multiple_of(chunk * size, size)

                def move(target):
                    copy = pltpu.make_async_copy(source, target, slot)
                    copy.wait() if wait else copy.start()

                if kind == "down":
                    total = outs[0].shape[0] // 2
                    move(outs[0].at[pl.ds(pl.multiple_of(group * total + row, size), size), :])
                elif kind == "up":
                    total = outs[0].shape[1] // 2
                    move(outs[0].at[pl.ds(row, size), pl.ds(group * total, total)])
                else:
                    width = outs[1].shape[0] // 2
                    per = width // size
                    quarter = chunk // per
                    inside = (chunk - quarter * per) * size
                    inner = pl.multiple_of(group * width + inside, size)

                    @pl.when(quarter < 3)
                    def _():
                        where = pl.multiple_of(quarter * 2 * width + inner, size)
                        move(outs[0].at[pl.ds(where, size), :])

                    @pl.when(quarter >= 3)
                    def _():
                        move(outs[1].at[pl.ds(inner, size), :])


def assemble(kind, count, me, pieces, shapes):
    anywhere = pl.BlockSpec(memory_space=pl.ANY)
    return pl.pallas_call(
        functools.partial(assemble_kernel, kind, count),
        in_specs=[pl.BlockSpec(memory_space=pltpu.SMEM)] + [anywhere] * 4,
        out_specs=[anywhere] * len(shapes),
        out_shape=[jax.ShapeDtypeStruct(shape, f32) for shape in shapes],
        scratch_shapes=[pltpu.SemaphoreType.DMA((2 * count,))],
        compiler_params=pltpu.CompilerParams(vmem_limit_bytes=2 << 20),
        cost_estimate=pl.CostEstimate(flops=0, bytes_accessed=7 << 20, transcendentals=0),
        name="assemble_" + kind,
    )(me, *pieces)


def per_device(
    size,
    tokens,
    cotangent,
    lengths,
    pad_mask,
    w_qkv,
    b_qkv,
    w_out,
    b_out,
    w_up,
    b_up,
    w_down,
    b_down,
    gain_one,
    shift_one,
    gain_two,
    shift_two,
):
    rows, model = tokens.shape
    width = w_qkv.shape[2]
    hidden = w_up.shape[1]
    count = min(16, size)
    bits = count.bit_length() - 1
    order_a = list(range(bits))
    order_b = order_a[:2][::-1] + order_a[2:]
    me_a, me_b = place_index(order_a), place_index(order_b)
    me = {0: me_a, 1: me_b}
    orders = {0: order_a, 1: order_b}

    frequency = np.float32(10000.0) ** (
        -(np.float32(2.0) * np.arange(HALF, dtype=np.float32)) / np.float32(HD)
    )
    angles = frequency.astype(np.float32)[:, None] * np.arange(rows, dtype=np.float32)[None, :]
    cosine = jnp.asarray(np.cos(angles.astype(np.float32)), f32)
    sine = jnp.asarray(np.sin(angles.astype(np.float32)), f32)
    row_of = lambda vec: vec.reshape(1, -1)
    swap = lambda values: lax.ppermute(values, "tensor", [(0, 1), (1, 0)])
    w_t = jnp.transpose(w_qkv, (1, 2, 0))

    hidden_one, q, k, v, att, lse, bias, mix = front(
        tokens,
        lengths,
        pad_mask,
        w_t,
        b_qkv,
        w_out,
        row_of(gain_one),
        row_of(shift_one),
        cosine,
        sine,
    )
    mix_other = swap(mix)
    me_ab = jnp.stack([me_a, me_b])
    me_ba = jnp.stack([me_b, me_a])
    resid, hidden_two, down, hid, d1k, d1s, u1k, u1s, gb_up1 = mlp(
        True,
        0,
        count,
        me_ab,
        (tokens, mix, mix_other, row_of(b_out), row_of(gain_two), row_of(shift_two)),
        cotangent,
        w_up,
        row_of(b_up),
        w_down,
    )
    down, hid, d2k, d2s, u2k, u2s, gb_up2 = mlp(
        False,
        1,
        count,
        me_ba,
        (hidden_two, down, hid),
        cotangent,
        w_up,
        row_of(b_up),
        w_down,
    )
    d1 = Chain(order_a, size, d1k, d1s)
    u1 = Chain(order_b, size, u1k, u1s)
    d2 = Chain(order_b, size, d2k, d2s)
    u2 = Chain(order_a, size, u2k, u2s)
    hid_other = swap(hid)
    grad_resid, low, grad_att, sums_two = middle(
        resid, hid, hid_other, cotangent, row_of(gain_two), w_out
    )
    down_other = swap(down)
    outputs = (resid + ((down + down_other) + b_down)).astype(bf16)
    rows_in = (q, k, v, att, grad_att)
    q1k, q1s, part, gb1 = attend_back(
        True, 0, count, me_ab[:1], rows_in, lse, bias, cosine, sine, w_t, hidden_one, low, None
    )
    q1 = Chain(order_a, size, q1k, q1s)
    q2k, q2s, part, gb2 = attend_back(
        False, 1, count, me_ba[:1], rows_in, lse, bias, cosine, sine, w_t, hidden_one, low, part
    )
    q2 = Chain(order_b, size, q2k, q2s)
    part_other = swap(part)
    grad_tokens, sums_one = last(tokens, part, part_other, grad_resid, row_of(gain_one))

    pad = model - 3 * width // 2
    small = jnp.concatenate(
        [
            sums_one[:2],
            sums_two[:4],
            jnp.pad(gb1[:1], ((0, 0), (0, pad))),
            jnp.pad(gb2[:1], ((0, 0), (0, pad))),
            gb_up1.reshape(-1, model),
            gb_up2.reshape(-1, model),
        ],
        axis=0,
    )
    for bit in range(size.bit_length() - 1):
        small = small + flip(small, bit, size)

    chains = [d1, u1, d2, u2, q1, q2]
    for chain in chains:
        chain.reduce()
    done = [chain.gather() for chain in chains]
    (grad_w_down,) = assemble("down", count, me_ab, done[0] + done[2], [(hidden, model)])
    (grad_w_up,) = assemble("up", count, me_ba, done[1] + done[3], [(model, hidden)])
    grad_w_qkv, grad_w_out = assemble(
        "attention", count, me_ab, done[4] + done[5], [(3 * width, model), (width, model)]
    )
    grad_w_qkv = jnp.transpose(grad_w_qkv.reshape(3, width, model), (2, 0, 1))
    grad_b_qkv = small[6:8, : 3 * width // 2].reshape(2, 3, width // 2)
    grad_b_qkv = jnp.transpose(grad_b_qkv, (1, 0, 2)).reshape(3, width)
    return (
        outputs,
        grad_tokens,
        grad_w_qkv,
        grad_b_qkv,
        grad_w_out,
        small[4],
        grad_w_up,
        small[8:].reshape(-1),
        grad_w_down,
        small[5],
        small[0],
        small[1],
        small[2],
        small[3],
    )


def solution(mesh):
    placed = (
        P("dp", None),
        P("dp", None),
        P("dp"),
        P("dp", None),
        P(None, None, "tensor"),
        P(None, "tensor"),
        P("tensor", None),
        P(),
        P(None, "tensor"),
        P("tensor"),
        P("tensor", None),
        P(),
        P(),
        P(),
        P(),
        P(),
    )
    return jax.shard_map(
        functools.partial(per_device, mesh.shape["dp"]),
        mesh=mesh,
        in_specs=placed,
        out_specs=(
            P("dp", None),
            P("dp", None),
            P(None, None, "tensor"),
            P(None, "tensor"),
            P("tensor", None),
            P(),
            P(None, "tensor"),
            P("tensor"),
            P("tensor", None),
            P(),
            P(),
            P(),
            P(),
            P(),
        ),
        check_vma=False,
    )
```

```python
import functools
import math

import jax
import jax.numpy as jnp
import numpy as np
from jax import lax
from jax.experimental import pallas as pl
from jax.experimental.pallas import tpu as pltpu
from jax.sharding import PartitionSpec as P

HD = 32
HALF = HD // 2
EPSILON = 1e-05
ROOT_HALF = 0.7071067811865476
ROOT_TWO_PI = 2.5066282746310002
LOG2E = math.log2(math.e)
HIDDEN_BIAS = -1e30
SAFE_POWER = 96.0
VMEM_BYTES = 60 << 20
PIECES = 1
ORDERS = ((0, 1, 2, 3), (1, 0, 2, 3))
LANES = 128
FREE = pl.CostEstimate(flops=0, bytes_accessed=0, transcendentals=0)
f32 = jnp.float32
bf16 = jnp.bfloat16


def dot_nn(a, b):
    return lax.dot_general(a, b, (((1,), (0,)), ((), ())), preferred_element_type=f32)


def dot_nt(a, b):
    return lax.dot_general(a, b, (((1,), (1,)), ((), ())), preferred_element_type=f32)


def dot_tn(a, b):
    return lax.dot_general(a, b, (((0,), (0,)), ((), ())), preferred_element_type=f32)


def normalize(values):
    centre = jnp.mean(values, axis=1, keepdims=True)
    shifted = values - centre
    inverse = lax.rsqrt(jnp.mean(shifted * shifted, axis=1, keepdims=True) + EPSILON)
    return shifted * inverse, inverse


def norm_back(grad_normed, normed, inverse, gain_vec):
    scaled = grad_normed * gain_vec
    first_mean = jnp.mean(scaled, axis=1, keepdims=True)
    second_mean = jnp.mean(scaled * normed, axis=1, keepdims=True)
    return inverse * (scaled - first_mean - normed * second_mean)


def split_three(values):
    first = values.astype(bf16)
    rest = values - first.astype(f32)
    second = rest.astype(bf16)
    third = (rest - second.astype(f32)).astype(bf16)
    return first, second, third


def stack_rows(*rows):
    count = rows[0].shape[1]
    place = lax.broadcasted_iota(jnp.int32, (16, count), 0)
    out = jnp.zeros((16, count), f32)
    for index, row in enumerate(rows):
        out = jnp.where(place == index, row, out)
    return out.astype(bf16)


def rope_rows(values, cosine, sine):
    heads = values.reshape(-1, 2, HALF, values.shape[1])
    lower, upper = heads[:, 0], heads[:, 1]
    turned = jnp.stack([lower * cosine - upper * sine, upper * cosine + lower * sine], axis=1)
    return turned.reshape(values.shape)


def rope_back_rows(values, cosine, sine):
    heads = values.reshape(-1, 2, HALF, values.shape[1])
    lower, upper = heads[:, 0], heads[:, 1]
    turned = jnp.stack([lower * cosine + upper * sine, upper * cosine - lower * sine], axis=1)
    return turned.reshape(values.shape)


def spread(me, count, keep_ref, send_ref, tiles):
    half = count // 2
    height = sum(source.shape[0] // count for source, _ in tiles)
    for place in range(count):
        chunk = jnp.bitwise_xor(me, place)
        target = keep_ref if place < half else send_ref
        start = (place % half) * height
        for source, tile in tiles:
            size = source.shape[0] // count
            rows = pl.ds(pl.multiple_of(chunk * size, 8), size)
            target[start : start + size, :] = source[rows, tile * LANES : (tile + 1) * LANES]
            start += size


def tiles_of(ref):
    return [(ref, tile) for tile in range(ref.shape[1] // LANES)]


def front_kernel(
    block,
    steps,
    heads,
    length_ref,
    tokens_ref,
    w_ref,
    b_ref,
    gain_ref,
    shift_ref,
    cos_ref,
    sin_ref,
    mask_ref,
    w_out_ref,
    hidden_ref,
    q_out,
    k_out,
    v_out,
    att_out,
    lse_ref,
    bias_ref,
    mix_ref,
    q_ref,
    k_ref,
    v_ref,
    att_ref,
):
    step = pl.program_id(0)
    seq_len = q_ref.shape[1]
    width = q_ref.shape[0]
    per_step = 2
    query_scale = HD ** (-0.5)

    @pl.when(step == 0)
    def _():
        place = lax.broadcasted_iota(jnp.int32, (1, seq_len), 1)
        visible = (place < length_ref[0]) & (mask_ref[...] == 1) | (place == 0)
        bias_ref[...] = jnp.where(visible, 0.0, HIDDEN_BIAS)

    @pl.when(step < steps)
    def _():
        normed, _ = normalize(tokens_ref[...].astype(f32))
        hidden = (normed * row_of(gain_ref) + row_of(shift_ref)).astype(bf16)
        hidden_ref[...] = hidden
        projected = dot_nt(w_ref[...].reshape(3 * width, w_ref.shape[2]), hidden)
        columns = pl.ds(pl.multiple_of(step * block, block), block)
        parts = []
        for index in range(3):
            column = jnp.broadcast_to(b_ref[index : index + 1, :], (128, width)).T
            column = jnp.concatenate([column] * (block // 128), axis=1)
            parts.append(projected[index * width : (index + 1) * width] + column)
        cosine, sine = cos_ref[...], sin_ref[...]
        query = (rope_rows(parts[0], cosine, sine) * query_scale).astype(bf16)
        key = rope_rows(parts[1], cosine, sine).astype(bf16)
        value = parts[2].astype(bf16)
        q_out[...], k_out[...], v_out[...] = query, key, value
        q_ref[:, columns], k_ref[:, columns], v_ref[:, columns] = query, key, value

    @pl.when((step >= steps) & (step < steps + heads // per_step))
    def _():
        ones = jnp.ones((1, seq_len), f32)
        key_extra = stack_rows(bias_ref[...])
        value_extra = stack_rows(ones)
        query_extra = stack_rows(ones)
        first_head = (step - steps) * per_step
        queries, keys, values, bounds = [], [], [], []
        for index in range(per_step):
            rows = pl.ds(pl.multiple_of((first_head + index) * HD, HD), HD)
            key = k_ref[rows, :]
            query = q_ref[rows, :].astype(f32) * LOG2E
            key_wide = key.astype(f32)
            bounds.append(
                jnp.max(jnp.sum(query * query, axis=0, keepdims=True))
                * jnp.max(jnp.sum(key_wide * key_wide, axis=0, keepdims=True))
            )
            queries.append(jnp.concatenate([*split_three(query), query_extra], axis=0))
            keys.append(jnp.concatenate([key, key, key, key_extra], axis=0))
            values.append(jnp.concatenate([v_ref[rows, :], value_extra], axis=0))
        bound = bounds[0]
        for other in bounds[1:]:
            bound = jnp.maximum(bound, other)

        def attend(shifted):
            size = min(512, seq_len)
            for index in range(per_step):
                head = first_head + index
                rows = pl.ds(pl.multiple_of(head * HD, HD), HD)
                for start in range(0, seq_len, size):
                    part = slice(start, start + size)
                    scores = dot_tn(keys[index], queries[index][:, part])
                    if shifted:
                        peak = jnp.max(scores, axis=0, keepdims=True)
                        powers = jnp.exp2(scores - peak)
                    else:
                        peak = 0.0
                        powers = jnp.exp2(scores)
                    summed = dot_nn(values[index], powers.astype(bf16))
                    total = summed[HD : HD + 1, :]
                    attended = (summed[:HD] * (1.0 / total)).astype(bf16)
                    att_ref[rows, part] = attended
                    att_out[index * HD : (index + 1) * HD, part] = attended
                    lse_ref[head, :, part] = peak + jnp.log(total) * LOG2E

        small = bound < SAFE_POWER * SAFE_POWER

        @pl.when(small)
        def _():
            attend(False)

        @pl.when(jnp.logical_not(small))
        def _():
            attend(True)

    @pl.when(step >= steps + heads // per_step)
    def _():
        size = mix_ref.shape[0]
        start = (step - (steps + heads // per_step)) * size
        columns = pl.ds(pl.multiple_of(start, size), size)
        mix_ref[...] = dot_tn(att_ref[:, columns], w_out_ref[...])


def row_of(ref):
    return ref[...].reshape(1, -1)


def const_spec(shape, index=None):
    where = tuple(index) if index is not None else (0,) * len(shape)
    return pl.BlockSpec(shape, lambda *_: where, pipeline_mode=pl.Buffered(1))


def out_spec(shape):
    where = (0,) * len(shape)
    return pl.BlockSpec(shape, lambda *_: where)


def front(tokens, lengths, pad_mask, w_t, b_qkv, w_out, gain_one, shift_one, cosine, sine):
    rows, model = tokens.shape
    width = w_t.shape[1]
    heads = width // HD
    block = min(256, rows)
    steps = rows // block
    turns = heads // 2
    tail = min(512, rows)
    clip = lambda i, low, high: jnp.clip(i - low, 0, high - 1)
    lanes = lambda i: (0, clip(i, 0, steps))
    return pl.pallas_call(
        functools.partial(front_kernel, block, steps, heads),
        grid=(steps + turns + rows // tail,),
        in_specs=[
            pl.BlockSpec(memory_space=pltpu.SMEM),
            pl.BlockSpec((block, model), lambda i: (clip(i, 0, steps), 0)),
            const_spec(w_t.shape),
            const_spec(b_qkv.shape),
            const_spec(gain_one.shape),
            const_spec(shift_one.shape),
            pl.BlockSpec((HALF, block), lanes),
            pl.BlockSpec((HALF, block), lanes),
            const_spec(pad_mask.shape),
            const_spec(w_out.shape),
        ],
        out_specs=[
            pl.BlockSpec((block, model), lambda i: (clip(i, 0, steps), 0)),
            pl.BlockSpec((width, block), lanes),
            pl.BlockSpec((width, block), lanes),
            pl.BlockSpec((width, block), lanes),
            pl.BlockSpec((2 * HD, rows), lambda i: (clip(i, steps, turns), 0)),
            out_spec((heads, 1, rows)),
            out_spec((1, rows)),
            pl.BlockSpec((tail, model), lambda i: (clip(i, steps + turns, rows // tail), 0)),
        ],
        out_shape=[
            jax.ShapeDtypeStruct((rows, model), bf16),
            jax.ShapeDtypeStruct((width, rows), bf16),
            jax.ShapeDtypeStruct((width, rows), bf16),
            jax.ShapeDtypeStruct((width, rows), bf16),
            jax.ShapeDtypeStruct((width, rows), bf16),
            jax.ShapeDtypeStruct((heads, 1, rows), f32),
            jax.ShapeDtypeStruct((1, rows), f32),
            jax.ShapeDtypeStruct((rows, model), f32),
        ],
        scratch_shapes=[pltpu.VMEM((width, rows), bf16)] * 4,
        compiler_params=pltpu.CompilerParams(vmem_limit_bytes=60 << 20),
        cost_estimate=FREE,
        name="front",
    )(lengths, tokens, w_t, b_qkv, gain_one, shift_one, cosine, sine, pad_mask, w_out)


def mlp_kernel(first, count, *refs):
    if first:
        me_ref, b_up_ref, b_out_ref, gain_ref, shift_ref, tokens_ref, own_ref, other_ref = refs[:8]
        refs = refs[8:]
    else:
        me_ref, b_up_ref, hidden_ref, act_in_ref, up_in_ref = refs[:5]
        refs = refs[5:]
    cot_ref, w_up_ref, w_down_ref = refs[:3]
    refs = refs[3:]
    if first:
        resid_ref, hidden_ref, act_ref, grad_up_ref = refs[:4]
    else:
        down_ref, hid_ref = refs[:2]
    keep_ref, send_ref, b_up_sum, wd_total, wu_total = refs[-5:]
    step = pl.program_id(0)

    @pl.when(step == 0)
    def _():
        wd_total[...] = jnp.zeros_like(wd_total)
        wu_total[...] = jnp.zeros_like(wu_total)
        b_up_sum[...] = jnp.zeros_like(b_up_sum)

    if first:
        resid = tokens_ref[...].astype(f32) + ((own_ref[...] + other_ref[...]) + row_of(b_out_ref))
        resid_ref[...] = resid
        normed, _ = normalize(resid)
        hidden = (normed * row_of(gain_ref) + row_of(shift_ref)).astype(bf16)
        hidden_ref[...] = hidden
    else:
        hidden = hidden_ref[...]
        before = slice(0, act_in_ref.shape[1])
        down_ref[...] = dot_nn(act_in_ref[...], w_down_ref[before, :])
        hid_ref[...] = dot_nt(up_in_ref[...], w_up_ref[:, before])
    cot = cot_ref[...]
    lead = 0 if first else act_in_ref.shape[1]
    units = wd_total.shape[0]
    b_up = row_of(b_up_ref)
    for start in range(0, units, 256):
        part = slice(start, min(start + 256, units))
        whole = slice(lead + part.start, lead + part.stop)
        w_up, w_down = w_up_ref[:, whole], w_down_ref[whole, :]
        upward = dot_nn(hidden, w_up) + b_up[:, whole]
        grad_act = dot_nt(cot, w_down)
        chance = 0.5 * (1.0 + lax.erf(upward * ROOT_HALF))
        activated = (upward * chance).astype(bf16)
        bell = jnp.exp2((-0.5 * LOG2E) * (upward * upward)) * (1.0 / ROOT_TWO_PI)
        grad_up = (grad_act * (chance + upward * bell)).astype(bf16)
        wd_total[part, :] += dot_tn(activated, cot)
        wu_total[:, part] += dot_tn(hidden, grad_up)
        b_up_sum[:, part] += jnp.sum(grad_up.astype(f32), axis=0, keepdims=True)
        if first:
            act_ref[:, part] = activated
            grad_up_ref[:, part] = grad_up
        else:
            down_ref[...] += dot_nn(activated, w_down)
            hid_ref[...] += dot_nt(grad_up, w_up)

    @pl.when(step == pl.num_programs(0) - 1)
    def _():
        spread(me_ref[0], count, keep_ref, send_ref, tiles_of(wd_total) + tiles_of(wu_total))


def mlp(first, units, count, me, b_up, extras, cotangent, w_up, w_down):
    rows, model = cotangent.shape
    block = min(256, rows)
    before = w_up.shape[1] - units
    row_spec = pl.BlockSpec((block, model), lambda i: (i, 0))
    unit_spec = lambda size: pl.BlockSpec((block, size), lambda i: (i, 0))
    in_specs = [pl.BlockSpec(memory_space=pltpu.SMEM)]
    in_specs += [const_spec(b_up.shape)]
    if first:
        in_specs += [const_spec((model,))] * 3 + [row_spec] * 3
    else:
        in_specs += [row_spec, unit_spec(before), unit_spec(before)]
    in_specs += [row_spec, const_spec(w_up.shape), const_spec(w_down.shape)]
    rows_f32 = jax.ShapeDtypeStruct((rows, model), f32)
    rows_b16 = jax.ShapeDtypeStruct((rows, model), bf16)
    units_b16 = jax.ShapeDtypeStruct((rows, units), bf16)
    piece = jax.ShapeDtypeStruct((units * model // LANES, LANES), f32)
    if first:
        out_shape = [rows_f32, rows_b16, units_b16, units_b16]
        out_specs = [row_spec, row_spec, unit_spec(units), unit_spec(units)]
    else:
        out_shape = [rows_f32, rows_f32]
        out_specs = [row_spec, row_spec]
    out_shape += [piece] * 2
    out_shape += [jax.ShapeDtypeStruct((1, units), f32)]
    out_specs += [out_spec(s.shape) for s in out_shape[len(out_specs) :]]
    return pl.pallas_call(
        functools.partial(mlp_kernel, first, count),
        grid=(rows // block,),
        in_specs=in_specs,
        out_specs=out_specs,
        out_shape=out_shape,
        scratch_shapes=[
            pltpu.VMEM((units, model), f32),
            pltpu.VMEM((model, units), f32),
        ],
        compiler_params=pltpu.CompilerParams(vmem_limit_bytes=34 << 20),
        cost_estimate=FREE,
        name="mlp_a" if first else "mlp_b",
    )(me, b_up, *extras, cotangent, w_up, w_down)


def piece_specs(pieces, row_spec):
    if len(pieces) == 1:
        return [row_spec]
    return [const_spec(pieces[0].shape)] * len(pieces)


def collect(step, refs, whole):
    if len(refs) == 1:
        whole[...] = refs[0][...]
        return
    size = refs[0].shape[0]
    per_step = whole.shape[0] // size
    for first in range(0, len(refs), per_step):

        @pl.when(step == first // per_step)
        def _():
            for index in range(per_step):
                whole[index * size : (index + 1) * size, :] = refs[first + index][...]


def middle_kernel(resid_ref, own_ref, cot_ref, gain_ref, w_out_ref, *refs):
    grad_resid_ref, low_ref, grad_att_ref, sums_ref, other_ref = refs[PIECES:]
    step = pl.program_id(0)
    collect(step, refs[:PIECES], other_ref)

    @pl.when(step == 0)
    def _():
        sums_ref[...] = jnp.zeros_like(sums_ref)

    normed, inverse = normalize(resid_ref[...])
    grad_hidden = own_ref[...] + other_ref[...]
    cot = cot_ref[...].astype(f32)
    grad_resid = cot + norm_back(grad_hidden, normed, inverse, row_of(gain_ref))
    low = grad_resid.astype(bf16)
    grad_resid_ref[...] = grad_resid
    low_ref[...] = low
    grad_att_ref[...] = dot_nt(w_out_ref[...], low).astype(bf16)
    sums_ref[0:1, :] += jnp.sum(grad_hidden * normed, axis=0, keepdims=True)
    sums_ref[1:2, :] += jnp.sum(grad_hidden, axis=0, keepdims=True)
    sums_ref[2:3, :] += jnp.sum(low.astype(f32), axis=0, keepdims=True)
    sums_ref[3:4, :] += jnp.sum(cot, axis=0, keepdims=True)


def middle(resid, own, other, cotangent, gain_two, w_out):
    rows, model = resid.shape
    width = w_out.shape[0]
    block = min(256, rows)
    row_spec = pl.BlockSpec((block, model), lambda i: (i, 0))
    return pl.pallas_call(
        middle_kernel,
        grid=(rows // block,),
        in_specs=[row_spec] * 3
        + [const_spec(gain_two.shape), const_spec(w_out.shape)]
        + piece_specs(other, row_spec),
        out_specs=[
            row_spec,
            row_spec,
            pl.BlockSpec((width, block), lambda i: (0, i)),
            out_spec((8, model)),
        ],
        out_shape=[
            jax.ShapeDtypeStruct((rows, model), f32),
            jax.ShapeDtypeStruct((rows, model), bf16),
            jax.ShapeDtypeStruct((width, rows), bf16),
            jax.ShapeDtypeStruct((8, model), f32),
        ],
        scratch_shapes=[pltpu.VMEM((block, model), f32)],
        compiler_params=pltpu.CompilerParams(vmem_limit_bytes=20 << 20),
        cost_estimate=FREE,
        name="middle",
    )(resid, own, cotangent, gain_two, w_out, *other)


def attend_back_kernel(
    q_ref,
    k_ref,
    v_ref,
    att_ref,
    grad_att_ref,
    lse_ref,
    bias_ref,
    cos_ref,
    sin_ref,
    grad_ref,
    query_sc,
    grads_sc,
    out_sc,
):
    seq_len = q_ref.shape[1]
    query_scale = HD ** (-0.5)
    ones = jnp.ones((1, seq_len), f32)
    size = min(256, seq_len)
    key_extra = stack_rows(bias_ref[...], ones, ones, ones)
    value_extra = stack_rows(ones, ones, ones)
    for head in range(1):
        rows = slice(0, HD)
        key, value, query_all = k_ref[rows, :], v_ref[rows, :], q_ref[rows, :]
        keys = jnp.concatenate([key, key, key, key_extra], axis=0)
        values = jnp.concatenate([value, value_extra], axis=0)
        grad_all = grad_att_ref[rows, :]
        inner_all = -jnp.sum(
            grad_all.astype(f32) * att_ref[rows, :].astype(f32), axis=0, keepdims=True
        )
        logs = [piece.astype(f32) for piece in split_three(-lse_ref[head])]
        inner = [piece.astype(f32) for piece in split_three(inner_all)]
        queries = jnp.concatenate(
            [*split_three(query_all.astype(f32) * LOG2E), stack_rows(ones, *logs)], axis=0
        )
        grads = jnp.concatenate([grad_all, stack_rows(*inner)], axis=0)
        query_sc[...] = queries
        grads_sc[...] = grads

        def turn(index, carry):
            grad_key, grad_value = carry
            for inner in range(2):
                start = pl.multiple_of((2 * index + inner) * size, size)
                part = pl.ds(start, size)
                chances = jnp.exp2(dot_tn(keys, query_sc[:, part]))
                grad_scores = (chances * dot_tn(values, grads_sc[:, part])).astype(bf16)
                grad_value = grad_value + dot_nt(grad_att_ref[:, part], chances.astype(bf16))
                grad_key = grad_key + dot_nt(q_ref[:, part], grad_scores)
                out_sc[:, part] = dot_nn(key, grad_scores) * query_scale
            return grad_key, grad_value

        nothing = jnp.zeros((HD, seq_len), f32)
        grad_key, grad_value = lax.fori_loop(
            0, seq_len // (2 * size), turn, (nothing, nothing)
        )
        grad_query = out_sc[...]
        cosine, sine = cos_ref[...], sin_ref[...]
        grad_ref[0, rows, :] = rope_back_rows(grad_query, cosine, sine).astype(bf16)
        grad_ref[1, rows, :] = rope_back_rows(grad_key, cosine, sine).astype(bf16)
        grad_ref[2, rows, :] = grad_value.astype(bf16)


def attend_back(index, per_call, rows_in, lse, bias, cosine, sine):
    rows = rows_in[0].shape[1]
    height = per_call * HD
    head_spec = pl.BlockSpec((HD, rows), lambda i: (index * per_call + i, 0))
    in_specs = [head_spec] * 5
    in_specs += [
        pl.BlockSpec((1, 1, rows), lambda i: (index * per_call + i, 0, 0)),
        const_spec((1, rows)),
        const_spec((HALF, rows)),
        const_spec((HALF, rows)),
    ]
    return pl.pallas_call(
        attend_back_kernel,
        grid=(per_call,),
        in_specs=in_specs,
        out_specs=pl.BlockSpec((3, HD, rows), lambda i: (0, i, 0)),
        out_shape=jax.ShapeDtypeStruct((3, height, rows), bf16),
        scratch_shapes=[
            pltpu.VMEM((3 * HD + 16, rows), bf16),
            pltpu.VMEM((HD + 16, rows), bf16),
            pltpu.VMEM((HD, rows), f32),
        ],
        compiler_params=pltpu.CompilerParams(vmem_limit_bytes=12 << 20),
        cost_estimate=FREE,
        name="attend_back",
    )(*rows_in, lse, bias, cosine, sine)


def pack_kernel(calls, lead, first, count, *refs):
    me_ref = refs[0]
    grad_refs = refs[1 : 1 + calls]
    att_ref, w_ref, hidden_ref, low_ref = refs[1 + calls : 5 + calls]
    refs = refs[5 + calls :]
    if first:
        keep_ref, send_ref, part_ref, b_ref, total_sc = refs
    else:
        part_in_ref, b_in_ref, sums_ref, b_up_a, b_up_b, tokens_ref = refs[:6]
        keep_ref, send_ref, part_ref, total_sc, small_sc = refs[6:]
    height = grad_refs[0].shape[1]
    seq_len = att_ref.shape[1]
    width = calls * height
    hidden = hidden_ref[...]
    ones = jnp.ones((8, seq_len), bf16)
    part = None if first else part_in_ref[...]
    b_sums = []
    for index in range(3):
        grads = jnp.concatenate([ref[index] for ref in grad_refs], axis=0)
        total_sc[index * width : (index + 1) * width, :] = dot_nn(grads, hidden)
        b_sums.append(dot_nt(ones, grads))
        more = dot_tn(grads, w_ref[index, lead : lead + width, :])
        part = more if part is None else part + more
    part_ref[...] = part
    total_sc[3 * width :, :] = dot_nn(att_ref[lead : lead + width, :], low_ref[...])
    tiles = tiles_of(total_sc)
    if first:
        for index in range(3):
            b_ref[index : index + 1, :width] = b_sums[index][:1]
    else:
        normed, _ = normalize(tokens_ref[...].astype(f32))
        rows = [
            jnp.sum(part * normed, axis=0, keepdims=True),
            jnp.sum(part, axis=0, keepdims=True),
            *[sums_ref[index : index + 1, :] for index in range(4)],
            b_up_a[...],
            b_up_b[...],
        ]
        place = 0
        for row in rows:
            for start in range(0, row.shape[1], LANES):
                small_sc[place : place + 1, :] = row[:, start : start + LANES]
                place += 1
        for index in range(3):
            both = [b_in_ref[index : index + 1, :lead], b_sums[index][:1]]
            both = jnp.concatenate(both, axis=1)
            spare = jnp.zeros((1, -both.shape[1] % LANES), f32)
            both = jnp.concatenate([both, spare], axis=1)
            for start in range(0, both.shape[1], LANES):
                small_sc[place : place + 1, :] = both[:, start : start + LANES]
                place += 1
        spare = small_sc.shape[0] - place
        if spare:
            small_sc[place:, :] = jnp.zeros((spare, LANES), f32)
        tiles = tiles + [(small_sc, 0)]
    spread(me_ref[0 if count > 4 else 1], count, keep_ref, send_ref, tiles)


def small_rows(model, width, units):
    per = -(-width // LANES)
    rows = (6 * model + units) // LANES + 3 * per
    return rows + -rows % 32


def pack(lead, count, me, grads, att, w_t, hidden, low, extra):
    first = not extra
    rows, model = hidden.shape
    calls, height = len(grads), grads[0].shape[1]
    width = calls * height
    in_specs = [pl.BlockSpec(memory_space=pltpu.SMEM)]
    in_specs += [const_spec(grads[0].shape)] * calls
    in_specs += [const_spec(v.shape) for v in (att, w_t, hidden, low, *extra)]
    total = 4 * width * model // LANES
    scratch = [pltpu.VMEM((4 * width, model), f32)]
    out_shape = [jax.ShapeDtypeStruct((rows, model), f32)]
    if first:
        out_shape.append(jax.ShapeDtypeStruct((8, width), f32))
    else:
        units = extra[3].shape[1] + extra[4].shape[1]
        small = small_rows(model, lead + width, units)
        scratch.append(pltpu.VMEM((small, LANES), f32))
        total += small
    out_shape = [jax.ShapeDtypeStruct((total // 2, LANES), f32)] * 2 + out_shape
    return pl.pallas_call(
        functools.partial(pack_kernel, calls, lead, first, count),
        grid=(1,),
        in_specs=in_specs,
        out_specs=[out_spec(s.shape) for s in out_shape],
        out_shape=out_shape,
        scratch_shapes=scratch,
        compiler_params=pltpu.CompilerParams(vmem_limit_bytes=30 << 20),
        cost_estimate=FREE,
        name="pack",
    )(me, *grads, att, w_t, hidden, low, *extra)


def last_kernel(tokens_ref, own_ref, grad_resid_ref, gain_ref, *refs):
    grad_ref, other_ref = refs[PIECES:]
    step = pl.program_id(0)
    collect(step, refs[:PIECES], other_ref)
    normed, inverse = normalize(tokens_ref[...].astype(f32))
    grad_hidden = own_ref[...] + other_ref[...]
    grad_ref[...] = grad_resid_ref[...] + norm_back(grad_hidden, normed, inverse, row_of(gain_ref))


def last(tokens, own, other, grad_resid, gain_one):
    rows, model = tokens.shape
    block = min(256, rows)
    row_spec = pl.BlockSpec((block, model), lambda i: (i, 0))
    return pl.pallas_call(
        last_kernel,
        grid=(rows // block,),
        in_specs=[row_spec] * 3 + [const_spec(gain_one.shape)] + piece_specs(other, row_spec),
        out_specs=row_spec,
        out_shape=jax.ShapeDtypeStruct((rows, model), f32),
        scratch_shapes=[pltpu.VMEM((block, model), f32)],
        compiler_params=pltpu.CompilerParams(vmem_limit_bytes=20 << 20),
        cost_estimate=FREE,
        name="last",
    )(tokens, own, grad_resid, gain_one, *other)


def finish_kernel(resid_ref, own_ref, bias_ref, *refs):
    out_ref, other_ref = refs[PIECES:]
    collect(pl.program_id(0), refs[:PIECES], other_ref)
    total = (own_ref[...] + other_ref[...]) + row_of(bias_ref)
    out_ref[...] = (resid_ref[...] + total).astype(bf16)


def finish(resid, own, other, b_down):
    rows, model = resid.shape
    block = min(256, rows)
    row_spec = pl.BlockSpec((block, model), lambda i: (i, 0))
    return pl.pallas_call(
        finish_kernel,
        grid=(rows // block,),
        in_specs=[row_spec] * 2 + [const_spec(b_down.shape)] + piece_specs(other, row_spec),
        out_specs=row_spec,
        out_shape=jax.ShapeDtypeStruct((rows, model), bf16),
        scratch_shapes=[pltpu.VMEM((block, model), f32)],
        compiler_params=pltpu.CompilerParams(vmem_limit_bytes=16 << 20),
        cost_estimate=FREE,
        name="finish",
    )(resid, own, b_down, *other)


def flip(values, bits, size):
    parts = len(bits)
    pairs = [
        (i * parts + j, (i ^ (1 << bits[j])) * parts + j) for i in range(size) for j in range(parts)
    ]
    return lax.ppermute(values, ("dp", "tensor"), pairs)


class Line:
    def __init__(self):
        self.token = jnp.zeros((), f32)

    def tie(self, values):
        values, self.token = lax.optimization_barrier((values, self.token))
        return values


class Chain:
    def __init__(self, line, size, halving, orders, keep, send):
        self.line, self.size = line, size
        self.keep, self.send = keep, send
        down = list(zip(*orders))
        rest = [(bit,) * len(orders) for bit in range(4, size.bit_length() - 1)]
        self.halving, self.whole = halving, down[halving:] + rest
        self.steps = down[:halving] + down[halving:] + down[:halving][::-1]
        self.middle = len(down)

    def start(self, phase):
        operand = self.line.tie(self.send)
        self.flying = flip(operand, self.steps[phase], self.size)

    def done(self, phase):
        got = self.line.tie(self.flying)
        if phase == len(self.steps) - 1:
            self.keep = got
        elif phase >= self.middle:
            self.send = jnp.concatenate([self.send, got], axis=0)
        else:
            total = (self.keep if phase < self.halving else self.send) + got
            if phase < self.halving - 1:
                self.keep, self.send = cut_two(total)
            else:
                self.send = total
            if phase == self.middle - 1:
                for bits in self.whole[self.middle - self.halving :]:
                    self.send = self.send + flip(self.send, bits, self.size)

    def result(self):
        return [self.send, self.keep]


def cut_two(values):
    half = values.shape[0] // 2
    return values[:half], values[half:]


def place_index(order):
    index = lax.axis_index("dp")
    out = jnp.zeros((), jnp.int32)
    for bit in order:
        out = out * 2 + jnp.bitwise_and(jnp.right_shift(index, bit), 1)
    return out


def feed_kernel(count, sizes, me_ref, *refs):
    pieces, (down_ref, up_ref) = refs[:-2], refs[-2:]
    half = count // 2
    lead = 0
    for group, units in enumerate(sizes):
        source = pieces[2 * group : 2 * group + 2]
        height = source[0].shape[0] // half
        sizes_of = (units // count, up_ref.shape[0] // count)
        for place in range(count):
            chunk = jnp.bitwise_xor(me_ref[0], place)
            start = (place % half) * height
            down_rows = pl.ds(pl.multiple_of(chunk * sizes_of[0] + lead, 8), sizes_of[0])
            up_rows = pl.ds(pl.multiple_of(chunk * sizes_of[1], 8), sizes_of[1])
            for target, rows, size, columns in (
                (down_ref, down_rows, sizes_of[0], range(0, down_ref.shape[1], LANES)),
                (up_ref, up_rows, sizes_of[1], range(lead, lead + units, LANES)),
            ):
                for column in columns:
                    target[rows, column : column + LANES] = source[place // half][
                        start : start + size, :
                    ]
                    start += size
        lead += units


def heads_kernel(groups, me_ref, *refs):
    pieces, outs = refs[:-12], refs[-12:]
    other_ref, pieces = pieces[-1], pieces[:-1]
    qkv_ref, out_ref, b_ref, b_up_ref = outs[:4]
    width = out_ref.shape[0]
    model = out_ref.shape[1]
    tiles = model // LANES
    lead = 0
    for group, (count, heads) in enumerate(groups):
        half = count // 2
        own = heads * HD
        size = 4 * own // count
        source = pieces[2 * group : 2 * group + 2]
        height = source[0].shape[0] // half
        for place in range(count):
            chunk = jnp.bitwise_xor(me_ref[0 if count > 4 else 1], place)
            section = chunk // (count // 4)
            inside = lead + (chunk - section * (count // 4)) * size
            begin = (place % half) * height

            def store(target, base):
                rows = pl.ds(pl.multiple_of(base, 8), size)
                for tile in range(tiles):
                    target[rows, tile * LANES : (tile + 1) * LANES] = source[place // half][
                        begin + tile * size : begin + (tile + 1) * size, :
                    ]

            @pl.when(section < 3)
            def _():
                store(qkv_ref, section * width + inside)

            @pl.when(section >= 3)
            def _():
                store(out_ref, inside)

        lead += own
    rest = height - tiles * size
    own_sc, other_sc = outs[-2:]
    for place in range(4):
        rows = pl.ds(pl.multiple_of(jnp.bitwise_xor(me_ref[1], place) * rest, 8), rest)
        begin = (place % 2) * height + tiles * size
        own_sc[rows, :] = source[place // 2][begin : begin + rest, :]
        rows = pl.ds(pl.multiple_of(jnp.bitwise_xor(me_ref[2], place) * rest, 8), rest)
        other_sc[rows, :] = other_ref[place * rest : (place + 1) * rest, :]
    vec_refs = outs[4:-2]
    for index, vec in enumerate(vec_refs):
        for tile in range(tiles):
            row = own_sc[index * tiles + tile, :]
            if index < 2:
                row = row + other_sc[index * tiles + tile, :]
            vec[tile * LANES : (tile + 1) * LANES] = row
    place = len(vec_refs) * tiles
    for tile in range(b_up_ref.shape[0] // LANES):
        b_up_ref[tile * LANES : (tile + 1) * LANES] = own_sc[place, :]
        place += 1
    per = -(-width // LANES)
    for index in range(3):
        for tile in range(per):
            stop = min(width, (tile + 1) * LANES)
            b_ref[index : index + 1, tile * LANES : stop] = own_sc[
                place : place + 1, : stop - tile * LANES
            ]
            place += 1


def assemble(kernel, me, pieces, shapes, scratch=()):
    return pl.pallas_call(
        kernel,
        grid=(1,),
        in_specs=[pl.BlockSpec(memory_space=pltpu.SMEM)] + [const_spec(p.shape) for p in pieces],
        out_specs=[out_spec(shape) for shape in shapes],
        out_shape=[jax.ShapeDtypeStruct(shape, f32) for shape in shapes],
        scratch_shapes=[pltpu.VMEM(shape, f32) for shape in scratch],
        compiler_params=pltpu.CompilerParams(vmem_limit_bytes=36 << 20),
        cost_estimate=FREE,
        name="assemble",
    )(me, *pieces)


def per_device(
    size,
    tokens,
    cotangent,
    lengths,
    pad_mask,
    w_qkv,
    b_qkv,
    w_out,
    b_out,
    w_up,
    b_up,
    w_down,
    b_down,
    gain_one,
    shift_one,
    gain_two,
    shift_two,
):
    rows, model = tokens.shape
    width = w_qkv.shape[2]
    hidden = w_up.shape[1]
    assert size >= 16 and size & (size - 1) == 0
    core = lax.axis_index("tensor")
    orders = ORDERS
    index_of = [[place_index(order[:bits]) for order in orders] for bits in (4, 2)]
    pick = lambda pair, flipped: jnp.where((core == 0) != flipped, pair[0], pair[1])
    me = jnp.stack(
        [pick(index_of[0], False), pick(index_of[1], False), pick(index_of[1], True)]
    )
    early = 2 * hidden // 5
    first_calls = 3

    frequency = np.float32(10000.0) ** (
        -(np.float32(2.0) * np.arange(HALF, dtype=np.float32)) / np.float32(HD)
    )
    angles = frequency.astype(np.float32)[:, None] * np.arange(rows, dtype=np.float32)[None, :]
    cosine = jnp.asarray(np.cos(angles.astype(np.float32)), f32)
    sine = jnp.asarray(np.sin(angles.astype(np.float32)), f32)
    swap = lambda values: lax.ppermute(values, "tensor", [(0, 1), (1, 0)])
    w_t = jnp.transpose(w_qkv, (1, 2, 0))
    line = Line()
    tie = line.tie
    at = {}

    def do_front():
        at["front"] = tie(
            front(
                tokens, lengths, pad_mask, w_t, b_qkv, w_out, gain_one, shift_one, cosine, sine
            )
        )
        at["mix"] = at["front"][-1]

    def do_mlp_a():
        extras = (tokens, at["mix"], *at["mix_other"])
        args = (16, me, b_up, (b_out, gain_two, shift_two, *tie(extras)), cotangent, w_up, w_down)
        at["mlp_a"] = out = tie(mlp(True, early, *args))
        at["a"] = Chain(line, size, 4, orders, *out[4:6])

    def do_mlp_b():
        args = (16, me, b_up, tie(at["mlp_a"][1:4]), cotangent, w_up, w_down)
        at["mlp_b"] = out = tie(mlp(False, hidden - early, *args))
        at["down"], at["hid"] = out[:2]
        at["b"] = Chain(line, size, 4, orders, *out[2:4])

    def do_middle():
        inputs = tie((at["mlp_a"][0], at["hid"], at["hid_other"]))
        at["middle"] = tie(middle(*inputs, cotangent, gain_two, w_out))

    def do_back(index):
        rows_in = (*at["front"][1:5], at["middle"][2])
        lse, bias = at["front"][5:7]
        at["back%d" % index] = tie(
            attend_back(index, 2, tie(rows_in), lse, bias, cosine, sine)
        )

    def do_pack(which):
        calls = range(width // (2 * HD))
        calls = calls[first_calls:] if which else calls[:first_calls]
        grads = [at["back%d" % index] for index in calls]
        halving = 2 if which else 4
        extra = ()
        if which:
            extra = (
                at["part"],
                at["pack0"][3],
                at["middle"][3],
                at["mlp_a"][-1],
                at["mlp_b"][-1],
                tokens,
            )
        at["pack%d" % which] = out = tie(
            pack(
                calls[0] * 2 * HD,
                1 << halving,
                me,
                tie(grads),
                at["front"][4],
                w_t,
                at["front"][0],
                at["middle"][1],
                extra,
            )
        )
        at["part"] = out[2]
        at["d" if which else "c"] = Chain(line, size, halving, orders, *out[:2])

    def do_last():
        inputs = tie((at["part"], at["part_other"], at["middle"][0]))
        at["last"] = tie(last(tokens, *inputs, gain_one))

    def do_finish():
        down, other = tie((at["down"], at["down_other"]))
        at["out"] = tie(finish(at["mlp_a"][0], down, other, b_down))

    def do_small():
        count = small_rows(model, width, hidden) // 4
        rest = [v for half in at["d"].result() for v in cut_two(half)]
        at["small"] = jnp.concatenate([v[-count:] for v in rest], axis=0)

    def swap_start(name):
        at[name + "_flying"] = [swap(tie(at[name]))]

    def swap_done(name):
        at[name + "_other"] = tie(at[name + "_flying"])

    def do_feed():
        pieces = at["a"].result() + at["b"].result()
        kernel = functools.partial(feed_kernel, 16, (early, hidden - early))
        at["feed"] = tie(assemble(kernel, me, tie(pieces), [(hidden, model), (model, hidden)]))

    def do_heads():
        pieces = at["c"].result() + at["d"].result() + at["small_other"]
        heads = width // HD
        split = (2 * first_calls, heads - 2 * first_calls)
        kernel = functools.partial(heads_kernel, tuple(zip((16, 4), split)))
        shapes = [(3 * width, model), (width, model), (3, width), (hidden,)] + [(model,)] * 6
        scratch = [(small_rows(model, width, hidden), LANES)] * 2
        at["heads"] = tie(assemble(kernel, me, tie(pieces), shapes, scratch))

    run_plan(locals())

    grad_w_down, grad_w_up = at["feed"]
    grad_w_qkv, grad_w_out, grad_b_qkv, grad_b_up, *vecs = at["heads"]
    grad_w_qkv = jnp.transpose(grad_w_qkv.reshape(3, width, model), (2, 0, 1))
    return (
        at["out"],
        at["last"],
        grad_w_qkv,
        grad_b_qkv,
        grad_w_out,
        vecs[4],
        grad_w_up,
        grad_b_up,
        grad_w_down,
        vecs[5],
        vecs[0],
        vecs[1],
        vecs[2],
        vecs[3],
    )


PLAN = (
    "front", "mix>", "mix<", "mlp_a", "a0>", "mlp_b", "a0<", "a1>", "hid>", "down>", "hid<",
    "b0>", "middle", "back", "0", "a1<", "a2>", "down<", "finish", "back", "1", "a2<", "a3>",
    "back", "2", "a3<", "b0<", "a4>", "b1>", "pack", "0", "c0>", "a4<", "a5>", "back", "3",
    "a5<", "a6>", "b1<", "b2>", "back", "4", "b2<", "b3>", "c0<", "c1>", "pack", "1", "d0>",
    "part>", "b3<", "b4>", "part<", "a6<", "a7>", "last", "c1<", "c2>", "b4<", "b5>", "d0<",
    "d1>", "c2<", "c3>", "a7<", "b5<", "b6>", "d1<", "d2>", "c3<", "c4>", "d2<", "d3>", "c4<",
    "c5>", "b6<", "b7>", "d3<", "d4>", "c5<", "c6>", "d4<", "d5>", "b7<", "feed", "c6<", "c7>",
    "d5<", "small", "small>", "small<", "c7<", "heads",
)


def run_plan(acts):
    at = acts["at"]
    names = iter(PLAN)
    for name in names:
        if name in ("back", "pack"):
            acts["do_" + name](int(next(names)))
        elif name[-1] not in "<>":
            acts["do_" + name]()
        elif name[:-1] in ("mix", "hid", "down", "part", "small"):
            acts["swap_start" if name[-1] == ">" else "swap_done"](name[:-1])
        else:
            chain = at[name[0]]
            (chain.start if name[-1] == ">" else chain.done)(int(name[1]))


def solution(mesh):
    placed = (
        P("dp", None),
        P("dp", None),
        P("dp"),
        P("dp", None),
        P(None, None, "tensor"),
        P(None, "tensor"),
        P("tensor", None),
        P(),
        P(None, "tensor"),
        P("tensor"),
        P("tensor", None),
        P(),
        P(),
        P(),
        P(),
        P(),
    )
    return jax.shard_map(
        functools.partial(per_device, mesh.shape["dp"]),
        mesh=mesh,
        in_specs=placed,
        out_specs=(
            P("dp", None),
            P("dp", None),
            P(None, None, "tensor"),
            P(None, "tensor"),
            P("tensor", None),
            P(),
            P(None, "tensor"),
            P("tensor"),
            P("tensor", None),
            P(),
            P(),
            P(),
            P(),
            P(),
        ),
        check_vma=False,
    )
```
